512 devices in a mesh: grid: 64 (over y, z_hi, core), vec: 8 (over x, z_lo).
Axes of the slice: x: 4, y: 8, z: 8 (z_hi: 4, z_lo: 2; z = z_hi * 2 + z_lo), core: 2. Of those that a mesh axis runs over, the one named last changes fastest.
Arguments:
- tgt_coords: float32 [3, 8192], P(None, 'grid'), may hold values from 0 to 1
- src_coords: float32 [3, 8192], P(None, 'grid'), may hold values from 0 to 1
- src_values: float32 [2048, 8192], P('vec', 'grid'), may hold values from -0.26516503 to 0.26516503
- grad_vectors: float32 [3, 2048, 8192], P(None, 'vec', 'grid'), may hold values from -0.75 to 0.75
Outputs:
- interaction: float32 [2048, 2048], P('grid', 'vec')
The draws below stay inside these ranges and needn't reach their ends.
All inputs are finite; a program needn't handle non-finite values.
Results may differ from the reference program's by a relative error of at most 0.00023.
Values sent between devices are 32-bit elements; how exact they have to be, the bound alone decides.
No kernel may reach another device: no remote copies, remote signals or barrier semaphores. Data moves between devices by JAX's collectives and lax.ppermute only.
A program may use at most 64 MiB of HBM per device.

```python
import math
import jax
import jax.numpy as jnp
from jax import lax

VECTORS = 2048
TARGETS = 8192
SOURCES = 8192


def raised(result, key, source, target, blocks, factor):
    def block_of(position):
        return (jnp.arange(result.shape[position]) // (result.shape[position] // blocks)).reshape((-1,) + (1,) * (result.ndim - 1 - position))

    one_side = jax.random.permutation(key, blocks)[block_of(target)]
    other_side = (block_of(target) + blocks // 2) % blocks
    return jnp.where((block_of(source) == one_side) | (block_of(source) == other_side), factor * result, result)


def block_levels(rng, extent, pieces, smallest, largest):
    factor_of = 1.0
    for dim, parts in pieces:
        draws = jax.random.uniform(jax.random.fold_in(jax.random.fold_in(rng, 6), dim), (parts,), jnp.float32, smallest / len(pieces), largest / len(pieces))
        factor_of = factor_of * jnp.repeat(jnp.exp(draws), extent[dim] // parts).reshape((-1,) + (1,) * (len(extent) - 1 - dim))
    return factor_of


def scatter_about(own_key, extent, width, reach, shards=(), held_as=jnp.bfloat16):
    result = width * jax.random.normal(own_key, extent, jnp.float32)
    if shards:
        result = result * block_levels(own_key, extent, shards, -0.22, 0.18)
    return jnp.clip(result, -reach, reach).astype(held_as)


def heavy_noise(rng, extent, width, bound, split, heavy, dtype=jnp.bfloat16):
    entries = width * jax.random.normal(rng, extent, jnp.float32)
    if split:
        entries = entries * block_levels(rng, extent, split, -0.22, 0.18)
    return jnp.clip(raised(entries, jax.random.fold_in(rng, 3), *heavy), -bound, bound).astype(dtype)


def setup_inputs(seed: int = 0) -> dict:
    keys = jax.random.split(jax.random.key(seed), 5)
    tgt_coords = jnp.clip(1.0 * jax.random.uniform(keys[0], (3, TARGETS), jnp.float32) ** block_levels(keys[0], (3, TARGETS), ((1, 64),), -0.2, 0.2), 0.0, 1.0)
    src_coords = jnp.clip(1.0 * jax.random.uniform(keys[1], (3, SOURCES), jnp.float32) ** block_levels(keys[1], (3, SOURCES), ((1, 64),), -0.2, 0.2), 0.0, 1.0)
    src_values = scatter_about(keys[2], (VECTORS, SOURCES), (4.0 * SOURCES ** -0.5), 0.26516503, ((0, 8), (1, 64)), jnp.float32)
    grad_vectors = heavy_noise(keys[3], (3, VECTORS, TARGETS), (4.0 * TARGETS ** -0.5), 0.75, ((1, 8), (2, 64)), (2, 1, 64, 4.0), jnp.float32)
    return {"tgt_coords": tgt_coords, "src_coords": src_coords, "src_values": src_values, "grad_vectors": grad_vectors}


stiff = 1.0
soft = 0.05

def pair_kernel(targets, sources):
    diff = targets[:, :, None] - sources[:, None, :]
    dist2 = lax.optimization_barrier(jnp.sum(diff * diff, axis=0))
    scale = 0.5 / ((1.0 + stiff * jnp.sqrt(dist2)) ** 2 * jnp.sqrt(dist2 + soft * soft))
    return diff * scale[None, :, :]

def reference(tgt_coords, src_coords, src_values, grad_vectors):
    block_len = math.gcd(TARGETS, 512)
    nblocks = TARGETS // block_len
    tgt_blocks = tgt_coords.reshape(3, nblocks, block_len).transpose(1, 0, 2)
    grad_blocks = grad_vectors.reshape(3, VECTORS, nblocks, block_len).transpose(2, 0, 1, 3)

    def step(total, items):
        tblock, gblock = items
        kern = pair_kernel(tblock, src_coords)
        partial_y = jnp.einsum('cts,qs->ctq', kern, src_values, precision=lax.Precision.HIGHEST)
        total = total + jnp.einsum('cpt,ctq->pq', gblock, partial_y, precision=lax.Precision.HIGHEST)
        return (total, None)
    total, _ = lax.scan(step, jnp.zeros((VECTORS, VECTORS), jnp.float32), (tgt_blocks, grad_blocks))
    return total
```

```python
import jax
import jax.numpy as jnp
from jax import lax
from jax.experimental import pallas as pl
from jax.experimental.pallas import tpu as pltpu
from jax.sharding import Mesh, PartitionSpec as P


SOFT2 = 0.05 * 0.05
TINY = 1e-30
GRID = ("yh", "y0", "h", "l", "c")
VEC = ("x", "zl")
SWAP = [(0, 1), (1, 0)]
BF16 = jnp.bfloat16


def copies(block, peers):
    return jnp.broadcast_to(block[None], (peers,) + block.shape)


def split(a):
    hi = a.astype(BF16)
    return hi, (a - hi.astype(jnp.float32)).astype(BF16)


def times_transposed(a, b):
    return lax.dot_general(a, b, (((1,), (1,)), ((), ())), preferred_element_type=jnp.float32)


def pair_matmul_kernel(origin_ref, own_ref, other_ref, src_ref, out_ref, hi_ref, lo_ref):
    blocks, _, half = own_ref.shape
    rows = out_ref.shape[1]
    origin = [origin_ref[comp : comp + 1, 0:1] for comp in range(3)]

    @pl.when(pl.program_id(0) == 0)
    def _():
        for j in range(blocks):
            for side, ref in enumerate((own_ref, other_ref)):
                cols = slice(side * half, (side + 1) * half)
                moment = None
                for comp in range(3):
                    g = ref[j, comp * rows : (comp + 1) * rows, :]
                    hi, lo = split(g)
                    hi_ref[j, (comp + 1) * rows : (comp + 2) * rows, cols] = hi
                    lo_ref[j, (comp + 1) * rows : (comp + 2) * rows, cols] = lo
                    tgt = ref[j, 3 * rows + comp : 3 * rows + comp + 1, :] - origin[comp]
                    moment = g * tgt if moment is None else moment + g * tgt
                hi, lo = split(moment)
                hi_ref[j, :rows, cols] = hi
                lo_ref[j, :rows, cols] = lo

    src = [src_ref[:, comp : comp + 1] for comp in range(3)]
    total = None
    for j in range(blocks):
        dist2 = None
        for comp in range(3):
            row = slice(3 * rows + comp, 3 * rows + comp + 1)
            tgt = jnp.concatenate([own_ref[j, row, :], other_ref[j, row, :]], axis=1)
            diff = tgt - src[comp]
            dist2 = diff * diff if dist2 is None else dist2 + diff * diff
        grow = 1.0 + dist2 * lax.rsqrt(jnp.maximum(dist2, TINY))
        grow2 = grow * grow
        hi, lo = split(lax.rsqrt((dist2 + SOFT2) * (grow2 * grow2)))
        part = times_transposed(hi, hi_ref[j]) + times_transposed(lo, hi_ref[j]) + times_transposed(hi, lo_ref[j])
        total = part if total is None else total + part
    z = total[:, :rows]
    for comp in range(3):
        z = z - (src[comp] - origin[comp]) * total[:, (comp + 1) * rows : (comp + 2) * rows]
    out_ref[0] = (0.5 * z).T


def pair_matmul(origin, own, other, src_cols, peers):
    blocks, height, half = own.shape
    rows = (height - 8) // 3
    total_s = src_cols.shape[0]
    per = total_s // peers
    step = 512
    inner = per // step
    pairs = total_s * 2 * half * blocks
    return pl.pallas_call(
        pair_matmul_kernel,
        out_shape=jax.ShapeDtypeStruct((peers, rows, per), jnp.float32),
        grid=(total_s // step,),
        in_specs=[
            pl.BlockSpec((8, half), lambda i: (0, 0)),
            pl.BlockSpec((blocks, height, half), lambda i: (0, 0, 0)),
            pl.BlockSpec((blocks, height, half), lambda i: (0, 0, 0)),
            pl.BlockSpec((step, 8), lambda i: (i, 0)),
        ],
        out_specs=pl.BlockSpec((1, rows, step), lambda i: (i // inner, 0, i % inner)),
        scratch_shapes=[pltpu.VMEM((blocks, 4 * rows, 2 * half), BF16)] * 2,
        compiler_params=pltpu.CompilerParams(
            dimension_semantics=("arbitrary",), vmem_limit_bytes=32 * 1024 * 1024
        ),
        cost_estimate=pl.CostEstimate(
            flops=pairs * 4 * rows * 2 * 3,
            bytes_accessed=2 * blocks * height * half * 4 + peers * rows * per * 4,
            transcendentals=2 * pairs,
        ),
    )(origin, own, other, src_cols)


def body(tgt_coords, src_coords, src_values, grad_vectors):
    n = {a: lax.axis_size(a) for a in GRID + VEC}
    nv = n["x"] * n["zl"]
    slab, pts = src_values.shape
    rows = slab // n["h"]
    zrows = rows // n["l"]
    piece = zrows // n["c"]
    h = lax.axis_index("h")
    c = lax.axis_index("c")

    grads = grad_vectors.reshape(3, n["h"], rows, pts)
    tail = jnp.concatenate([tgt_coords, jnp.zeros((5, pts), jnp.float32)], axis=0)
    first, second = (jnp.concatenate([grads[:, k].reshape(3 * rows, pts), tail], axis=0) for k in range(2))
    mine = jnp.where(h == 0, first, second)
    theirs = jnp.where(h == 0, second, first)
    from_z = lax.ppermute(theirs, "h", SWAP)
    from_diag = lax.ppermute(theirs, ("y0", "h"), [(i, 3 - i) for i in range(4)])
    from_y = lax.ppermute(mine, "y0", SWAP)

    src_pad = jnp.concatenate([src_coords, jnp.zeros((5, pts), jnp.float32)], axis=0)
    nsrc = n["yh"] * n["h"] * n["l"]
    src_all = lax.all_to_all(copies(src_pad, nsrc), ("yh", "h", "l"), 0, 0, tiled=True)
    src_cols = src_all.transpose(0, 2, 1).reshape(nsrc * pts, 8)
    origin = jnp.broadcast_to(jnp.mean(src_all, axis=(0, 2))[:, None], (8, pts))

    own = jnp.stack([mine, from_y, from_z, from_diag])
    other = lax.ppermute(own, "c", SWAP)

    partial_z = pair_matmul(origin, own, other, src_cols, n["yh"])
    src_values, partial_z = lax.optimization_barrier((src_values, partial_z))

    spts = partial_z.shape[2]
    arrived = lax.all_to_all(
        partial_z.reshape(n["yh"] * n["l"], zrows, spts), ("yh", "l"), 0, 0, tiled=True
    )
    v_l = lax.ppermute(src_values, "l", SWAP)
    v_h = lax.ppermute(src_values, "h", SWAP)
    v_hl = lax.ppermute(src_values, ("h", "l"), [(i, 3 - i) for i in range(4)])
    me = lax.axis_index(("h", "l"))
    stack = jnp.stack([src_values, v_l, v_h, v_hl])
    values = jnp.concatenate([lax.dynamic_index_in_dim(stack, me ^ b, 0, False) for b in range(4)], axis=1)

    z = arrived.sum(axis=0)
    z_all = lax.all_to_all(copies(z, nv), VEC, 0, 0, tiled=True).reshape(nv, n["c"], piece, spts)

    def product(core):
        zc = lax.dynamic_index_in_dim(z_all, core, 1, False).reshape(nv * piece, spts)
        return lax.dot_general(zc, values, (((1,), (1,)), ((), ())), precision=lax.Precision.HIGH)

    part = lax.ppermute(product(1 - c), "c", SWAP) + product(c)
    back = lax.all_to_all(part.reshape(nv, piece, slab), ("yh", "y0"), 0, 0, tiled=True)
    return back.sum(axis=0)


def solution(mesh):
    fine = Mesh(mesh.devices.reshape(4, 2, 2, 2, 2, 4, 2), GRID + VEC)

    return jax.shard_map(
        body,
        mesh=fine,
        in_specs=(P(None, GRID), P(None, GRID), P(VEC, GRID), P(None, VEC, GRID)),
        out_specs=P(GRID, VEC),
        check_vma=False,
    )
```

```python
import jax
import jax.numpy as jnp
from jax import lax
from jax.experimental import pallas as pl
from jax.experimental.pallas import tpu as pltpu
from jax.sharding import Mesh, PartitionSpec as P


SOFT2 = 0.05 * 0.05
TINY = 1e-30
GRID = ("yh", "y0", "h", "l", "c")
VEC = ("x", "zl")
SWAP = [(0, 1), (1, 0)]
BF16 = jnp.bfloat16
TAIL = 8


def copies(block, peers):
    return jnp.broadcast_to(block[None], (peers,) + block.shape)


def split(a):
    hi = a.astype(BF16)
    return hi, (a - hi.astype(jnp.float32)).astype(BF16)


def times_transposed(a, b):
    return lax.dot_general(a, b, (((1,), (1,)), ((), ())), preferred_element_type=jnp.float32)


def pair_matmul_kernel(origin_ref, own_ref, other_ref, src_ref, out_ref, hi_ref, lo_ref):
    blocks, _, half = own_ref.shape
    rows = out_ref.shape[1]
    origin = [origin_ref[comp : comp + 1, 0:1] for comp in range(3)]

    @pl.when(pl.program_id(0) == 0)
    def _():
        for j in range(blocks):
            for side, ref in enumerate((own_ref, other_ref)):
                cols = slice(side * half, (side + 1) * half)
                moment = None
                for comp in range(3):
                    g = ref[j, comp * rows : (comp + 1) * rows, :]
                    hi, lo = split(g)
                    hi_ref[j, (comp + 1) * rows : (comp + 2) * rows, cols] = hi
                    lo_ref[j, (comp + 1) * rows : (comp + 2) * rows, cols] = lo
                    tgt = ref[j, 3 * rows + comp : 3 * rows + comp + 1, :] - origin[comp]
                    moment = g * tgt if moment is None else moment + g * tgt
                hi, lo = split(moment)
                hi_ref[j, :rows, cols] = hi
                lo_ref[j, :rows, cols] = lo

    src = [src_ref[:, comp : comp + 1] for comp in range(3)]
    total = None
    for j in range(blocks):
        dist2 = None
        for comp in range(3):
            row = slice(3 * rows + comp, 3 * rows + comp + 1)
            tgt = jnp.concatenate([own_ref[j, row, :], other_ref[j, row, :]], axis=1)
            diff = tgt - src[comp]
            dist2 = diff * diff if dist2 is None else dist2 + diff * diff
        grow = 1.0 + dist2 * lax.rsqrt(jnp.maximum(dist2, TINY))
        grow2 = grow * grow
        hi, lo = split(lax.rsqrt((dist2 + SOFT2) * (grow2 * grow2)))
        part = times_transposed(hi, hi_ref[j]) + times_transposed(lo, hi_ref[j]) + times_transposed(hi, lo_ref[j])
        total = part if total is None else total + part
    z = total[:, :rows]
    for comp in range(3):
        z = z - (src[comp] - origin[comp]) * total[:, (comp + 1) * rows : (comp + 2) * rows]
    out_ref[0] = (0.5 * z).T


def pair_matmul(origin, own, other, src_cols, peers):
    blocks, height, half = own.shape
    rows = (height - TAIL) // 3
    total_s = src_cols.shape[0]
    per = total_s // peers
    step = STEP
    inner = per // step
    pairs = total_s * 2 * half * blocks
    return pl.pallas_call(
        pair_matmul_kernel,
        out_shape=jax.ShapeDtypeStruct((peers, rows, per), jnp.float32),
        grid=(total_s // step,),
        in_specs=[
            pl.BlockSpec((8, half), lambda i: (0, 0)),
            pl.BlockSpec((blocks, height, half), lambda i: (0, 0, 0)),
            pl.BlockSpec((blocks, height, half), lambda i: (0, 0, 0)),
            pl.BlockSpec((step, 8), lambda i: (i, 0)),
        ],
        out_specs=pl.BlockSpec((1, rows, step), lambda i: (i // inner, 0, i % inner)),
        scratch_shapes=[pltpu.VMEM((blocks, 4 * rows, 2 * half), BF16)] * 2,
        compiler_params=pltpu.CompilerParams(
            dimension_semantics=("arbitrary",), vmem_limit_bytes=32 * 1024 * 1024
        ),
        cost_estimate=pl.CostEstimate(
            flops=pairs * 4 * rows * 2 * 3,
            bytes_accessed=2 * blocks * height * half * 4 + peers * rows * per * 4,
            transcendentals=2 * pairs,
        ),
    )(origin, own, other, src_cols)


STEP = 512


def body(tgt_coords, src_coords, src_values, grad_vectors):
    n = {a: lax.axis_size(a) for a in GRID + VEC}
    nz = n["h"] * n["l"]
    nv = n["x"] * n["zl"]
    slab, pts = src_values.shape
    rows = slab // nz
    piece = rows // n["c"]
    c = lax.axis_index("c")

    grads = grad_vectors.reshape(3, nz, rows, pts).transpose(1, 0, 2, 3).reshape(nz, 3 * rows, pts)
    tail = jnp.concatenate([tgt_coords, src_coords, jnp.zeros((TAIL - 6, pts), jnp.float32)], axis=0)
    load = jnp.concatenate([grads, copies(tail, nz)], axis=1)
    load = copies(load, n["y0"]).reshape(n["y0"] * nz, 3 * rows + TAIL, pts)
    own = lax.all_to_all(load, ("y0", "h", "l"), 0, 0, tiled=True)
    other = lax.ppermute(own, "c", SWAP)

    near = own[:, 3 * rows + 3 : 3 * rows + 6, :].reshape(n["y0"], 3 * nz, pts)
    near = lax.dynamic_index_in_dim(near, lax.axis_index("y0"), 0, False)
    near = jnp.pad(near, ((0, 4), (0, 0)))
    src_all = lax.all_to_all(copies(near, n["yh"]), "yh", 0, 0, tiled=True)
    src_all = src_all[:, : 3 * nz].reshape(n["yh"] * nz, 3, pts)
    src_cols = src_all.transpose(0, 2, 1).reshape(n["yh"] * nz * pts, 3)
    src_cols = jnp.pad(src_cols, ((0, 0), (0, 5)))
    origin = jnp.mean(src_all, axis=(0, 2))
    origin = jnp.broadcast_to(jnp.pad(origin, (0, 5))[:, None], (8, pts))
    src_values, src_cols = lax.optimization_barrier((src_values, src_cols))

    values = lax.all_to_all(copies(src_values, nz), ("h", "l"), 0, 0, tiled=True)

    partial_z = pair_matmul(origin, own, other, src_cols, n["yh"])
    spts = partial_z.shape[2]
    partial_z, values = lax.optimization_barrier((partial_z, values))

    arrived = lax.all_to_all(partial_z, "yh", 0, 0, tiled=True)
    z = arrived.sum(axis=0)
    z_all = lax.all_to_all(copies(z, nv), VEC, 0, 0, tiled=True).reshape(nv, n["c"], piece, spts)
    values = values.transpose(1, 0, 2).reshape(slab, spts)

    def product(core):
        zc = lax.dynamic_index_in_dim(z_all, core, 1, False).reshape(nv * piece, spts)
        return lax.dot_general(zc, values, (((1,), (1,)), ((), ())), precision=lax.Precision.HIGH)

    part = lax.ppermute(product(1 - c), "c", SWAP) + product(c)
    back = lax.all_to_all(part.reshape(nv, piece, slab), ("yh", "y0"), 0, 0, tiled=True)
    return back.sum(axis=0)


def solution(mesh):
    fine = Mesh(mesh.devices.reshape(4, 2, 2, 2, 2, 4, 2), GRID + VEC)

    return jax.shard_map(
        body,
        mesh=fine,
        in_specs=(P(None, GRID), P(None, GRID), P(VEC, GRID), P(None, VEC, GRID)),
        out_specs=P(GRID, VEC),
        check_vma=False,
    )
```

```python
import jax
import jax.numpy as jnp
from jax import lax
from jax.experimental.layout import Layout, with_layout_constraint
from jax.experimental import pallas as pl
from jax.experimental.pallas import tpu as pltpu
from jax.sharding import Mesh, PartitionSpec as P


SOFT2 = 0.05 * 0.05
TINY = 1e-30
GRID = ("yh", "y0", "h", "l", "c")
VEC = ("x", "zl")
SWAP = [(0, 1), (1, 0)]
BF16 = jnp.bfloat16
TAIL = 16
DEPTH = 128


def copies(block, peers):
    return jnp.broadcast_to(block[None], (peers,) + block.shape)


def split(a):
    hi = a.astype(BF16)
    return hi, (a - hi.astype(jnp.float32)).astype(BF16)


def times_transposed(a, b):
    return lax.dot_general(a, b, (((1,), (1,)), ((), ())), preferred_element_type=jnp.float32)


def pieces(a):
    first = a.astype(BF16).astype(jnp.float32)
    second = (a - first).astype(BF16).astype(jnp.float32)
    return first, second, a - first - second


def dist_rows(points, factor, mine):
    p = [factor * x for x in pieces(points)]
    norm = points[0:1] * points[0:1] + points[1:2] * points[1:2] + points[2:3] * points[2:3]
    n = list(pieces(norm))
    one = [jnp.ones_like(norm)] * 3
    if mine:
        rows = [p[0], p[0], p[1], p[1], p[0], p[2]] + n + one
    else:
        rows = [p[0], p[1], p[0], p[1], p[2], p[0]] + one + n
    rows.append(jnp.zeros((DEPTH - 24, points.shape[1]), jnp.float32))
    return jnp.concatenate(rows, axis=0)


def pair_matmul_kernel(origin_ref, own_ref, other_ref, src_ref, out_ref, hi_ref, lo_ref, tgt_ref):
    blocks, _, half = own_ref.shape
    rows = out_ref.shape[1]
    origin = origin_ref[0:3, 0:1]

    @pl.when(pl.program_id(0) == 0)
    def _():
        for j in range(blocks):
            for side, ref in enumerate((own_ref, other_ref)):
                cols = slice(side * half, (side + 1) * half)
                tgt = ref[j, 3 * rows : 3 * rows + 3, :] - origin
                tgt_ref[j, :, cols] = dist_rows(tgt, 1.0, False).astype(BF16)
                moment = None
                for comp in range(3):
                    g = ref[j, comp * rows : (comp + 1) * rows, :]
                    hi, lo = split(g)
                    hi_ref[j, (comp + 1) * rows : (comp + 2) * rows, cols] = hi
                    lo_ref[j, (comp + 1) * rows : (comp + 2) * rows, cols] = lo
                    part = g * tgt[comp : comp + 1]
                    moment = part if moment is None else moment + part
                hi, lo = split(moment)
                hi_ref[j, :rows, cols] = hi
                lo_ref[j, :rows, cols] = lo

    points = src_ref[0, 0:3, :] - origin
    src_rows = dist_rows(points, -2.0, True).T.astype(BF16)
    src_cols = src_ref[0].T
    total = None
    for j in range(blocks):
        dist2 = jnp.dot(src_rows, tgt_ref[j], preferred_element_type=jnp.float32)
        dist2 = jnp.maximum(dist2, TINY)
        grow = 1.0 + dist2 * lax.rsqrt(dist2)
        grow2 = grow * grow
        hi, lo = split(lax.rsqrt((dist2 + SOFT2) * (grow2 * grow2)))
        part = times_transposed(hi, hi_ref[j]) + times_transposed(lo, hi_ref[j]) + times_transposed(hi, lo_ref[j])
        total = part if total is None else total + part
    z = total[:, :rows]
    for comp in range(3):
        away = src_cols[:, comp : comp + 1] - origin_ref[comp : comp + 1, 0:1]
        z = z - away * total[:, (comp + 1) * rows : (comp + 2) * rows]
    out_ref[0] = (0.5 * z).T


def pair_matmul(origin, own, other, src):
    blocks, height, half = own.shape
    rows = (height - TAIL) // 3
    peers, _, per = src.shape
    pairs = peers * per * 2 * half * blocks
    return pl.pallas_call(
        pair_matmul_kernel,
        out_shape=jax.ShapeDtypeStruct((peers, rows, per), jnp.float32),
        grid=(peers,),
        in_specs=[
            pl.BlockSpec((8, half), lambda i: (0, 0)),
            pl.BlockSpec((blocks, height, half), lambda i: (0, 0, 0)),
            pl.BlockSpec((blocks, height, half), lambda i: (0, 0, 0)),
            pl.BlockSpec((1, 8, per), lambda i: (i, 0, 0)),
        ],
        out_specs=pl.BlockSpec((1, rows, per), lambda i: (i, 0, 0)),
        scratch_shapes=[
            pltpu.VMEM((blocks, 4 * rows, 2 * half), BF16),
            pltpu.VMEM((blocks, 4 * rows, 2 * half), BF16),
            pltpu.VMEM((blocks, DEPTH, 2 * half), BF16),
        ],
        compiler_params=pltpu.CompilerParams(
            dimension_semantics=("arbitrary",), vmem_limit_bytes=32 * 1024 * 1024
        ),
        cost_estimate=pl.CostEstimate(
            flops=pairs * (4 * rows * 2 * 3 + 2 * DEPTH),
            bytes_accessed=2 * blocks * height * half * 4 + peers * rows * per * 4,
            transcendentals=2 * pairs,
        ),
    )(origin, own, other, src)


def body(tgt_coords, src_coords, src_values, grad_vectors):
    n = {a: lax.axis_size(a) for a in GRID + VEC}
    nz = n["h"] * n["l"]
    nv = n["x"] * n["zl"]
    slab, pts = src_values.shape
    rows = slab // nz
    piece = rows // n["c"]
    c = lax.axis_index("c")

    own_src = jnp.pad(src_coords, ((0, 5), (0, 0)))
    src_y = lax.all_to_all(copies(own_src, n["yh"]), "yh", 0, 0, tiled=True)
    src_y = src_y[:, :3].reshape(3 * n["yh"], pts)

    grads = grad_vectors.reshape(3, nz, rows, pts).transpose(1, 0, 2, 3).reshape(nz, 3 * rows, pts)
    tail = jnp.concatenate([tgt_coords, src_y, jnp.zeros((1, pts), jnp.float32)], axis=0)
    load = jnp.concatenate([grads, copies(tail, nz)], axis=1)
    load = copies(load, n["y0"]).reshape(n["y0"] * nz, 3 * rows + TAIL, pts)
    own = lax.all_to_all(load, ("y0", "h", "l"), 0, 0, tiled=True)
    src_values, own = lax.optimization_barrier((src_values, own))
    other = lax.ppermute(own, "c", SWAP)

    near = own[:, 3 * rows + 3 : 3 * rows + 3 + 3 * n["yh"], :].reshape(n["y0"], nz, n["yh"], 3, pts)
    near = lax.dynamic_index_in_dim(near, lax.axis_index("y0"), 0, False)
    src = near.transpose(1, 2, 0, 3).reshape(n["yh"], 3, nz * pts)
    src = jnp.pad(src, ((0, 0), (0, 5), (0, 0)))
    origin = jnp.broadcast_to(jnp.mean(src, axis=(0, 2))[:, None], (8, pts))

    rowmajor = Layout(major_to_minor=(0, 1, 2))
    load = with_layout_constraint(copies(src_values, nz), rowmajor)
    values = with_layout_constraint(lax.all_to_all(load, ("h", "l"), 0, 0, tiled=True), rowmajor)

    partial_z = pair_matmul(origin, own, other, src)
    spts = partial_z.shape[2]
    partial_z, values = lax.optimization_barrier((partial_z, values))

    arrived = lax.all_to_all(partial_z, "yh", 0, 0, tiled=True)
    z = arrived.sum(axis=0)
    z_all = lax.all_to_all(copies(z, nv), VEC, 0, 0, tiled=True).reshape(nv, n["c"], piece, spts)
    values = values.transpose(1, 0, 2).reshape(slab, spts)

    def product(core):
        zc = lax.dynamic_index_in_dim(z_all, core, 1, False).reshape(nv * piece, spts)
        return lax.dot_general(zc, values, (((1,), (1,)), ((), ())), precision=lax.Precision.HIGH)

    part = lax.ppermute(product(1 - c), "c", SWAP) + product(c)
    back = lax.all_to_all(part.reshape(nv, piece, slab), ("yh", "y0"), 0, 0, tiled=True)
    return back.sum(axis=0)


def solution(mesh):
    fine = Mesh(mesh.devices.reshape(4, 2, 2, 2, 2, 4, 2), GRID + VEC)

    return jax.shard_map(
        body,
        mesh=fine,
        in_specs=(P(None, GRID), P(None, GRID), P(VEC, GRID), P(None, VEC, GRID)),
        out_specs=P(GRID, VEC),
        check_vma=False,
    )
```

```python
import jax
import jax.numpy as jnp
from jax import lax
from jax.experimental import pallas as pl
from jax.experimental.pallas import tpu as pltpu
from jax.sharding import Mesh, PartitionSpec as P


SOFT2 = 0.05 * 0.05
TINY = 1e-30
GRID = ("yh", "y0", "h", "l", "c")
VEC = ("x", "zl")
SWAP = [(0, 1), (1, 0)]
BF16 = jnp.bfloat16
TAIL = 16


def copies(block, peers):
    return jnp.broadcast_to(block[None], (peers,) + block.shape)


def split(a):
    hi = a.astype(BF16)
    return hi, (a - hi.astype(jnp.float32)).astype(BF16)


def times_transposed(a, b):
    return lax.dot_general(a, b, (((1,), (1,)), ((), ())), preferred_element_type=jnp.float32)


def pair_matmul_kernel(*refs):
    origin_ref, own_ref, other_ref, src_ref, *earlier, out_ref, hi_ref, lo_ref = refs
    blocks, _, half = own_ref.shape
    rows = out_ref.shape[1]
    origin = [origin_ref[comp : comp + 1, 0:1] for comp in range(3)]

    @pl.when(pl.program_id(0) == 0)
    def _():
        for j in range(blocks):
            for side, ref in enumerate((own_ref, other_ref)):
                cols = slice(side * half, (side + 1) * half)
                moment = None
                for comp in range(3):
                    g = ref[j, comp * rows : (comp + 1) * rows, :]
                    hi, lo = split(g)
                    hi_ref[j, (comp + 1) * rows : (comp + 2) * rows, cols] = hi
                    lo_ref[j, (comp + 1) * rows : (comp + 2) * rows, cols] = lo
                    tgt = ref[j, 3 * rows + comp : 3 * rows + comp + 1, :] - origin[comp]
                    moment = g * tgt if moment is None else moment + g * tgt
                hi, lo = split(moment)
                hi_ref[j, :rows, cols] = hi
                lo_ref[j, :rows, cols] = lo

    src_cols = src_ref[0].T
    src = [src_cols[:, comp : comp + 1] for comp in range(3)]
    total = None
    for j in range(blocks):
        dist2 = None
        for comp in range(3):
            row = slice(3 * rows + comp, 3 * rows + comp + 1)
            tgt = jnp.concatenate([own_ref[j, row, :], other_ref[j, row, :]], axis=1)
            diff = tgt - src[comp]
            dist2 = diff * diff if dist2 is None else dist2 + diff * diff
        grow = 1.0 + dist2 * lax.rsqrt(jnp.maximum(dist2, TINY))
        grow2 = grow * grow
        hi, lo = split(lax.rsqrt((dist2 + SOFT2) * (grow2 * grow2)))
        part = times_transposed(hi, hi_ref[j]) + times_transposed(lo, hi_ref[j]) + times_transposed(hi, lo_ref[j])
        total = part if total is None else total + part
    z = total[:, :rows]
    for comp in range(3):
        z = z - (src[comp] - origin[comp]) * total[:, (comp + 1) * rows : (comp + 2) * rows]
    z = (0.5 * z).T
    for ref in earlier:
        z = z + ref[0]
    out_ref[0] = z


def pair_matmul(origin, own, other, src, *earlier):
    blocks, height, half = own.shape
    rows = (height - TAIL) // 3
    peers, _, per = src.shape
    pairs = peers * per * 2 * half * blocks
    return pl.pallas_call(
        pair_matmul_kernel,
        out_shape=jax.ShapeDtypeStruct((peers, rows, per), jnp.float32),
        grid=(peers,),
        in_specs=[
            pl.BlockSpec((8, half), lambda i: (0, 0)),
            pl.BlockSpec((blocks, height, half), lambda i: (0, 0, 0)),
            pl.BlockSpec((blocks, height, half), lambda i: (0, 0, 0)),
            pl.BlockSpec((1, 8, per), lambda i: (i, 0, 0)),
        ]
        + [pl.BlockSpec((1, rows, per), lambda i: (i, 0, 0))] * len(earlier),
        out_specs=pl.BlockSpec((1, rows, per), lambda i: (i, 0, 0)),
        scratch_shapes=[
            pltpu.VMEM((blocks, 4 * rows, 2 * half), BF16),
            pltpu.VMEM((blocks, 4 * rows, 2 * half), BF16),
        ],
        compiler_params=pltpu.CompilerParams(
            dimension_semantics=("arbitrary",), vmem_limit_bytes=32 * 1024 * 1024
        ),
        cost_estimate=pl.CostEstimate(
            flops=pairs * 4 * rows * 2 * 3,
            bytes_accessed=2 * blocks * height * half * 4 + peers * rows * per * 4,
            transcendentals=2 * pairs,
        ),
    )(origin, own, other, src, *earlier)


def body(tgt_coords, src_coords, src_values, grad_vectors):
    n = {a: lax.axis_size(a) for a in GRID + VEC}
    nz = n["h"] * n["l"]
    nv = n["x"] * n["zl"]
    slab, pts = src_values.shape
    rows = slab // nz
    piece = rows // n["c"]
    c = lax.axis_index("c")

    own_src = jnp.pad(src_coords, ((0, 5), (0, 0)))
    src_y = lax.all_to_all(copies(own_src, n["yh"]), "yh", 0, 0, tiled=True)
    src_y = src_y[:, :3].reshape(3 * n["yh"], pts)

    grads = grad_vectors.reshape(3, nz, rows, pts).transpose(1, 0, 2, 3).reshape(nz, 3 * rows, pts)
    tail = jnp.concatenate([tgt_coords, src_y, jnp.zeros((1, pts), jnp.float32)], axis=0)
    load = jnp.concatenate([grads, copies(tail, nz)], axis=1)
    own = lax.all_to_all(load, ("h", "l"), 0, 0, tiled=True)
    far = lax.ppermute(own, "y0", SWAP)
    own_other = lax.ppermute(own, "c", SWAP)

    near = own[:, 3 * rows + 3 : 3 * rows + 3 + 3 * n["yh"], :].reshape(nz, n["yh"], 3, pts)
    src = near.transpose(1, 2, 0, 3).reshape(n["yh"], 3, nz * pts)
    src = jnp.pad(src, ((0, 0), (0, 5), (0, 0)))
    origin = jnp.broadcast_to(jnp.mean(src, axis=(0, 2))[:, None], (8, pts))

    partial_z = pair_matmul(origin, own, own_other, src)
    far_other = lax.ppermute(far, "c", SWAP)
    partial_z = pair_matmul(origin, far, far_other, src, partial_z)
    spts = partial_z.shape[2]
    src_values, partial_z = lax.optimization_barrier((src_values, partial_z))

    arrived = lax.all_to_all(partial_z, "yh", 0, 0, tiled=True)
    v_l = lax.ppermute(src_values, "l", SWAP)
    v_h = lax.ppermute(src_values, "h", SWAP)
    v_hl = lax.ppermute(src_values, ("h", "l"), [(i, 3 - i) for i in range(4)])
    me = lax.axis_index(("h", "l"))
    stack = jnp.stack([src_values, v_l, v_h, v_hl])
    values = jnp.concatenate([lax.dynamic_index_in_dim(stack, me ^ b, 0, False) for b in range(4)], axis=1)
    z = arrived.sum(axis=0)
    z_all = lax.all_to_all(copies(z, nv), VEC, 0, 0, tiled=True).reshape(nv, n["c"], piece, spts)

    def product(core):
        zc = lax.dynamic_index_in_dim(z_all, core, 1, False).reshape(nv * piece, spts)
        return lax.dot_general(zc, values, (((1,), (1,)), ((), ())), precision=lax.Precision.HIGH)

    part = lax.ppermute(product(1 - c), "c", SWAP) + product(c)
    back = lax.all_to_all(part.reshape(nv, piece, slab), ("yh", "y0"), 0, 0, tiled=True)
    return back.sum(axis=0)


def solution(mesh):
    fine = Mesh(mesh.devices.reshape(4, 2, 2, 2, 2, 4, 2), GRID + VEC)

    return jax.shard_map(
        body,
        mesh=fine,
        in_specs=(P(None, GRID), P(None, GRID), P(VEC, GRID), P(None, VEC, GRID)),
        out_specs=P(GRID, VEC),
        check_vma=False,
    )
```

```python
import jax
import jax.numpy as jnp
from jax import lax
from jax.experimental.layout import Layout, with_layout_constraint
from jax.experimental import pallas as pl
from jax.experimental.pallas import tpu as pltpu
from jax.sharding import Mesh, PartitionSpec as P


SOFT2 = 0.05 * 0.05
TINY = 1e-30
GRID = ("yh", "y0", "h", "l", "c")
VEC = ("x", "zl")
SWAP = [(0, 1), (1, 0)]
BF16 = jnp.bfloat16
TAIL = 8


def copies(block, peers):
    return jnp.broadcast_to(block[None], (peers,) + block.shape)


def split(a):
    hi = a.astype(BF16)
    return hi, (a - hi.astype(jnp.float32)).astype(BF16)


def times_transposed(a, b):
    return lax.dot_general(a, b, (((1,), (1,)), ((), ())), preferred_element_type=jnp.float32)


def pair_matmul_kernel(first_ref, origin_ref, own_ref, other_ref, src_ref, out_ref, hi_ref, lo_ref):
    blocks, _, half = own_ref.shape
    rows = out_ref.shape[1]
    origin = [origin_ref[comp : comp + 1, 0:1] for comp in range(3)]

    @pl.when(pl.program_id(0) == 0)
    def _():
        for j in range(blocks):
            for side, ref in enumerate((own_ref, other_ref)):
                cols = slice(side * half, (side + 1) * half)
                moment = None
                for comp in range(3):
                    g = ref[j, comp * rows : (comp + 1) * rows, :]
                    hi, lo = split(g)
                    hi_ref[j, (comp + 1) * rows : (comp + 2) * rows, cols] = hi
                    lo_ref[j, (comp + 1) * rows : (comp + 2) * rows, cols] = lo
                    tgt = ref[j, 3 * rows + comp : 3 * rows + comp + 1, :] - origin[comp]
                    moment = g * tgt if moment is None else moment + g * tgt
                hi, lo = split(moment)
                hi_ref[j, :rows, cols] = hi
                lo_ref[j, :rows, cols] = lo

    src_cols = src_ref[0].T
    src = [src_cols[:, comp : comp + 1] for comp in range(3)]
    total = None
    for j in range(blocks):
        dist2 = None
        for comp in range(3):
            row = slice(3 * rows + comp, 3 * rows + comp + 1)
            tgt = jnp.concatenate([own_ref[j, row, :], other_ref[j, row, :]], axis=1)
            diff = tgt - src[comp]
            dist2 = diff * diff if dist2 is None else dist2 + diff * diff
        grow = 1.0 + dist2 * lax.rsqrt(jnp.maximum(dist2, TINY))
        grow2 = grow * grow
        hi, lo = split(lax.rsqrt((dist2 + SOFT2) * (grow2 * grow2)))
        part = times_transposed(hi, hi_ref[j]) + times_transposed(lo, hi_ref[j]) + times_transposed(hi, lo_ref[j])
        total = part if total is None else total + part
    z = total[:, :rows]
    for comp in range(3):
        z = z - (src[comp] - origin[comp]) * total[:, (comp + 1) * rows : (comp + 2) * rows]
    out_ref[0] = (0.5 * z).T


def pair_matmul(first, origin, own, other, src):
    blocks, height, half = own.shape
    rows = (height - TAIL) // 3
    peers, _, per = src.shape
    pairs = peers * per * 2 * half * blocks
    return pl.pallas_call(
        pair_matmul_kernel,
        out_shape=jax.ShapeDtypeStruct((peers, rows, per), jnp.float32),
        grid_spec=pltpu.PrefetchScalarGridSpec(
            num_scalar_prefetch=1,
            grid=(peers,),
            in_specs=[
                pl.BlockSpec((8, half), lambda i, f: (0, 0)),
                pl.BlockSpec((blocks, height, half), lambda i, f: (0, 0, 0)),
                pl.BlockSpec((blocks, height, half), lambda i, f: (0, 0, 0)),
                pl.BlockSpec((1, 8, per), lambda i, f: (i, 0, 0)),
            ],
            out_specs=pl.BlockSpec((1, rows, per), lambda i, f: ((i + f[0]) % peers, 0, 0)),
            scratch_shapes=[
                pltpu.VMEM((blocks, 4 * rows, 2 * half), BF16),
                pltpu.VMEM((blocks, 4 * rows, 2 * half), BF16),
            ],
        ),
        compiler_params=pltpu.CompilerParams(
            dimension_semantics=("arbitrary",), vmem_limit_bytes=32 * 1024 * 1024
        ),
        cost_estimate=pl.CostEstimate(
            flops=pairs * 4 * rows * 2 * 3,
            bytes_accessed=2 * blocks * height * half * 4 + peers * rows * per * 4,
            transcendentals=2 * pairs,
        ),
    )(first, origin, own, other, src)


def body(tgt_coords, src_coords, src_values, grad_vectors):
    n = {a: lax.axis_size(a) for a in GRID + VEC}
    nz = n["h"] * n["l"]
    nv = n["x"] * n["zl"]
    slab, pts = src_values.shape
    rows = slab // nz
    piece = rows // n["c"]
    c = lax.axis_index("c")

    grads = grad_vectors.reshape(3, nz, rows, pts).transpose(1, 0, 2, 3).reshape(nz, 3 * rows, pts)
    tail = jnp.concatenate([tgt_coords, src_coords, jnp.zeros((TAIL - 6, pts), jnp.float32)], axis=0)
    load = jnp.concatenate([grads, copies(tail, nz)], axis=1)
    load = copies(load, n["y0"]).reshape(n["y0"] * nz, 3 * rows + TAIL, pts)
    own = lax.all_to_all(load, ("y0", "h", "l"), 0, 0, tiled=True)
    other = lax.ppermute(own, "c", SWAP)

    near = own[:, 3 * rows + 3 : 3 * rows + 6, :].reshape(n["y0"], nz, 3, pts)
    near = lax.dynamic_index_in_dim(near, lax.axis_index("y0"), 0, False)
    near = jnp.pad(near.transpose(1, 0, 2).reshape(3, nz * pts), ((0, 5), (0, 0)))
    ny = n["yh"]
    ring = [near]
    for k in range(1, ny):
        ring.append(lax.ppermute(near, "yh", [((i + k) % ny, i) for i in range(ny)]))
    src = jnp.stack(ring)
    first = lax.axis_index("yh").astype(jnp.int32).reshape(1)
    origin = jnp.broadcast_to(jnp.mean(src, axis=(0, 2))[:, None], (8, pts))
    src_values, src = lax.optimization_barrier((src_values, src))

    rowmajor = Layout(major_to_minor=(0, 1, 2))
    load = with_layout_constraint(copies(src_values, nz), rowmajor)
    values = with_layout_constraint(lax.all_to_all(load, ("h", "l"), 0, 0, tiled=True), rowmajor)

    partial_z = pair_matmul(first, origin, own, other, src)
    spts = partial_z.shape[2]
    partial_z, values = lax.optimization_barrier((partial_z, values))

    arrived = lax.all_to_all(partial_z, "yh", 0, 0, tiled=True)
    z = arrived.sum(axis=0)
    z_all = lax.all_to_all(copies(z, nv), VEC, 0, 0, tiled=True).reshape(nv, n["c"], piece, spts)

    values = values.transpose(1, 0, 2).reshape(slab, spts)

    def product(core):
        zc = lax.dynamic_index_in_dim(z_all, core, 1, False).reshape(nv * piece, spts)
        return lax.dot_general(zc, values, (((1,), (1,)), ((), ())), precision=lax.Precision.HIGH)

    part = lax.ppermute(product(1 - c), "c", SWAP) + product(c)
    back = lax.all_to_all(part.reshape(nv, piece, slab), ("yh", "y0"), 0, 0, tiled=True)
    return back.sum(axis=0)


def solution(mesh):
    fine = Mesh(mesh.devices.reshape(4, 2, 2, 2, 2, 4, 2), GRID + VEC)

    return jax.shard_map(
        body,
        mesh=fine,
        in_specs=(P(None, GRID), P(None, GRID), P(VEC, GRID), P(None, VEC, GRID)),
        out_specs=P(GRID, VEC),
        check_vma=False,
    )
```

```python
import jax
import jax.numpy as jnp
from jax import lax
from jax.experimental.layout import Layout, with_layout_constraint
from jax.experimental import pallas as pl
from jax.experimental.pallas import tpu as pltpu
from jax.sharding import Mesh, PartitionSpec as P


SOFT2 = 0.05 * 0.05
TINY = 1e-30
GRID = ("yh", "y0", "h", "l", "c")
VEC = ("x", "zl")
SWAP = [(0, 1), (1, 0)]
BF16 = jnp.bfloat16
TAIL = 16


def copies(block, peers):
    return jnp.broadcast_to(block[None], (peers,) + block.shape)


def split(a):
    hi = a.astype(BF16)
    return hi, (a - hi.astype(jnp.float32)).astype(BF16)


def times_transposed(a, b):
    return lax.dot_general(a, b, (((1,), (1,)), ((), ())), preferred_element_type=jnp.float32)


def pair_matmul_kernel(origin_ref, own_ref, other_ref, src_ref, out_ref, hi_ref, lo_ref):
    blocks, _, half = own_ref.shape
    rows = out_ref.shape[1]
    origin = [origin_ref[comp : comp + 1, 0:1] for comp in range(3)]

    @pl.when(pl.program_id(0) == 0)
    def _():
        for j in range(blocks):
            for side, ref in enumerate((own_ref, other_ref)):
                cols = slice(side * half, (side + 1) * half)
                moment = None
                for comp in range(3):
                    g = ref[j, comp * rows : (comp + 1) * rows, :]
                    hi, lo = split(g)
                    hi_ref[j, (comp + 1) * rows : (comp + 2) * rows, cols] = hi
                    lo_ref[j, (comp + 1) * rows : (comp + 2) * rows, cols] = lo
                    tgt = ref[j, 3 * rows + comp : 3 * rows + comp + 1, :] - origin[comp]
                    moment = g * tgt if moment is None else moment + g * tgt
                hi, lo = split(moment)
                hi_ref[j, :rows, cols] = hi
                lo_ref[j, :rows, cols] = lo

    src_cols = src_ref[0].T
    src = [src_cols[:, comp : comp + 1] for comp in range(3)]
    total = None
    for j in range(blocks):
        dist2 = None
        for comp in range(3):
            row = slice(3 * rows + comp, 3 * rows + comp + 1)
            tgt = jnp.concatenate([own_ref[j, row, :], other_ref[j, row, :]], axis=1)
            diff = tgt - src[comp]
            dist2 = diff * diff if dist2 is None else dist2 + diff * diff
        grow = 1.0 + dist2 * lax.rsqrt(jnp.maximum(dist2, TINY))
        grow2 = grow * grow
        hi, lo = split(lax.rsqrt((dist2 + SOFT2) * (grow2 * grow2)))
        part = times_transposed(hi, hi_ref[j]) + times_transposed(lo, hi_ref[j]) + times_transposed(hi, lo_ref[j])
        total = part if total is None else total + part
    z = total[:, :rows]
    for comp in range(3):
        z = z - (src[comp] - origin[comp]) * total[:, (comp + 1) * rows : (comp + 2) * rows]
    out_ref[0] = (0.5 * z).T


def pair_matmul(origin, own, other, src):
    blocks, height, half = own.shape
    rows = (height - TAIL) // 3
    peers, _, per = src.shape
    pairs = peers * per * 2 * half * blocks
    return pl.pallas_call(
        pair_matmul_kernel,
        out_shape=jax.ShapeDtypeStruct((peers, rows, per), jnp.float32),
        grid=(peers,),
        in_specs=[pl.BlockSpec(memory_space=pltpu.VMEM)] * 3 + [pl.BlockSpec((1, 8, per), lambda i: (i, 0, 0))],
        out_specs=pl.BlockSpec((1, rows, per), lambda i: (i, 0, 0)),
        scratch_shapes=[pltpu.VMEM((blocks, 4 * rows, 2 * half), BF16)] * 2,
        compiler_params=pltpu.CompilerParams(
            dimension_semantics=("arbitrary",), vmem_limit_bytes=32 * 1024 * 1024
        ),
        cost_estimate=pl.CostEstimate(
            flops=pairs * 4 * rows * 2 * 3,
            bytes_accessed=2 * blocks * height * half * 4 + peers * rows * per * 4,
            transcendentals=2 * pairs,
        ),
    )(origin, own, other, src)


def body(tgt_coords, src_coords, src_values, grad_vectors):
    n = {a: lax.axis_size(a) for a in GRID + VEC}
    nz = n["h"] * n["l"]
    nv = n["x"] * n["zl"]
    slab, pts = src_values.shape
    rows = slab // nz
    piece = rows // n["c"]
    c = lax.axis_index("c")

    src_y = lax.all_to_all(copies(src_coords, n["yh"]), "yh", 0, 0, tiled=True)
    src_y = src_y.reshape(3 * n["yh"], pts)
    rowmajor = Layout(major_to_minor=(0, 1, 2))
    values = with_layout_constraint(copies(src_values, nz), rowmajor)

    grads = grad_vectors.reshape(3, nz, rows, pts).transpose(1, 0, 2, 3).reshape(nz, 3 * rows, pts)
    tail = jnp.concatenate([tgt_coords, src_y, jnp.zeros((1, pts), jnp.float32)], axis=0)
    load = jnp.concatenate([grads, copies(tail, nz)], axis=1)
    load = copies(load, n["y0"]).reshape(n["y0"] * nz, 3 * rows + TAIL, pts)
    own = lax.all_to_all(load, ("y0", "h", "l"), 0, 0, tiled=True)
    values, own = lax.optimization_barrier((values, own))
    other = lax.ppermute(own, "c", SWAP)

    near = own[:, 3 * rows + 3 : 3 * rows + 3 + 3 * n["yh"], :].reshape(n["y0"], nz, n["yh"], 3, pts)
    near = lax.dynamic_index_in_dim(near, lax.axis_index("y0"), 0, False)
    src = near.transpose(1, 2, 0, 3).reshape(n["yh"], 3, nz * pts)
    src = jnp.pad(src, ((0, 0), (0, 5), (0, 0)))
    origin = jnp.broadcast_to(jnp.mean(src, axis=(0, 2))[:, None], (8, pts))

    values = with_layout_constraint(lax.all_to_all(values, ("h", "l"), 0, 0, tiled=True), rowmajor)

    partial_z = pair_matmul(origin, own, other, src)
    spts = partial_z.shape[2]
    partial_z, values = lax.optimization_barrier((partial_z, values))

    arrived = lax.all_to_all(partial_z, "yh", 0, 0, tiled=True)
    z = arrived.sum(axis=0)
    z_all = lax.all_to_all(copies(z, nv), VEC, 0, 0, tiled=True).reshape(nv, n["c"], piece, spts)
    values = values.transpose(1, 0, 2).reshape(slab, spts)

    def product(core):
        zc = lax.dynamic_index_in_dim(z_all, core, 1, False).reshape(nv * piece, spts)
        return lax.dot_general(zc, values, (((1,), (1,)), ((), ())), precision=lax.Precision.HIGH)

    part = lax.ppermute(product(1 - c), "c", SWAP) + product(c)
    back = lax.all_to_all(part.reshape(nv, piece, slab), ("yh", "y0"), 0, 0, tiled=True)
    return back.sum(axis=0)


def solution(mesh):
    fine = Mesh(mesh.devices.reshape(4, 2, 2, 2, 2, 4, 2), GRID + VEC)

    return jax.shard_map(
        body,
        mesh=fine,
        in_specs=(P(None, GRID), P(None, GRID), P(VEC, GRID), P(None, VEC, GRID)),
        out_specs=P(GRID, VEC),
        check_vma=False,
    )
```

```python
import jax
import jax.numpy as jnp
from jax import lax
from jax.experimental.layout import Layout, with_layout_constraint
from jax.experimental import pallas as pl
from jax.experimental.pallas import tpu as pltpu
from jax.sharding import Mesh, PartitionSpec as P


SOFT2 = 0.05 * 0.05
TINY = 1e-30
GRID = ("yh", "y0", "h", "l", "c")
VEC = ("x", "zl")
SWAP = [(0, 1), (1, 0)]
BF16 = jnp.bfloat16
TAIL = 16


def copies(block, peers):
    return jnp.broadcast_to(block[None], (peers,) + block.shape)


def split(a):
    hi = a.astype(BF16)
    return hi, (a - hi.astype(jnp.float32)).astype(BF16)


def times_transposed(a, b):
    return lax.dot_general(a, b, (((1,), (1,)), ((), ())), preferred_element_type=jnp.float32)


def pair_matmul_kernel(origin_ref, own_ref, other_ref, src_ref, out_ref, hi_ref, lo_ref):
    blocks, _, half = own_ref.shape
    rows = out_ref.shape[1]
    origin = [origin_ref[comp : comp + 1, 0:1] for comp in range(3)]

    @pl.when(pl.program_id(0) == 0)
    def _():
        for j in range(blocks):
            for side, ref in enumerate((own_ref, other_ref)):
                cols = slice(side * half, (side + 1) * half)
                moment = None
                for comp in range(3):
                    g = ref[j, comp * rows : (comp + 1) * rows, :]
                    hi, lo = split(g)
                    hi_ref[j, (comp + 1) * rows : (comp + 2) * rows, cols] = hi
                    lo_ref[j, (comp + 1) * rows : (comp + 2) * rows, cols] = lo
                    tgt = ref[j, 3 * rows + comp : 3 * rows + comp + 1, :] - origin[comp]
                    moment = g * tgt if moment is None else moment + g * tgt
                hi, lo = split(moment)
                hi_ref[j, :rows, cols] = hi
                lo_ref[j, :rows, cols] = lo

    src_cols = src_ref[0].T
    src = [src_cols[:, comp : comp + 1] for comp in range(3)]
    total = None
    for j in range(blocks):
        dist2 = None
        for comp in range(3):
            row = slice(3 * rows + comp, 3 * rows + comp + 1)
            tgt = jnp.concatenate([own_ref[j, row, :], other_ref[j, row, :]], axis=1)
            diff = tgt - src[comp]
            dist2 = diff * diff if dist2 is None else dist2 + diff * diff
        grow = 1.0 + dist2 * lax.rsqrt(jnp.maximum(dist2, TINY))
        grow2 = grow * grow
        hi, lo = split(lax.rsqrt((dist2 + SOFT2) * (grow2 * grow2)))
        part = times_transposed(hi, hi_ref[j]) + times_transposed(lo, hi_ref[j]) + times_transposed(hi, lo_ref[j])
        total = part if total is None else total + part
    z = total[:, :rows]
    for comp in range(3):
        z = z - (src[comp] - origin[comp]) * total[:, (comp + 1) * rows : (comp + 2) * rows]
    out_ref[0] = (0.5 * z).T


def pair_matmul(origin, own, other, src):
    blocks, height, half = own.shape
    rows = (height - TAIL) // 3
    peers, _, per = src.shape
    pairs = peers * per * 2 * half * blocks
    return pl.pallas_call(
        pair_matmul_kernel,
        out_shape=jax.ShapeDtypeStruct((peers, rows, per), jnp.float32),
        grid=(peers,),
        in_specs=[pl.BlockSpec(memory_space=pltpu.VMEM)] * 3 + [pl.BlockSpec((1, 8, per), lambda i: (i, 0, 0))],
        out_specs=pl.BlockSpec((1, rows, per), lambda i: (i, 0, 0)),
        scratch_shapes=[pltpu.VMEM((blocks, 4 * rows, 2 * half), BF16)] * 2,
        compiler_params=pltpu.CompilerParams(
            dimension_semantics=("arbitrary",), vmem_limit_bytes=32 * 1024 * 1024
        ),
        cost_estimate=pl.CostEstimate(
            flops=pairs * 4 * rows * 2 * 3,
            bytes_accessed=2 * blocks * height * half * 4 + peers * rows * per * 4,
            transcendentals=2 * pairs,
        ),
    )(origin, own, other, src)


def body(tgt_coords, src_coords, src_values, grad_vectors):
    n = {a: lax.axis_size(a) for a in GRID + VEC}
    nz = n["h"] * n["l"]
    nv = n["x"] * n["zl"]
    slab, pts = src_values.shape
    rows = slab // nz
    piece = rows // n["c"]
    c = lax.axis_index("c")

    src_y = lax.all_to_all(copies(src_coords, n["yh"]), "yh", 0, 0, tiled=True)
    src_y = src_y.reshape(3 * n["yh"], pts)
    rowmajor = Layout(major_to_minor=(0, 1, 2))
    values = with_layout_constraint(copies(src_values, nz), rowmajor)

    grads = grad_vectors.reshape(3, nz, rows, pts).transpose(1, 0, 2, 3).reshape(nz, 3 * rows, pts)
    tail = jnp.concatenate([tgt_coords, src_y, jnp.zeros((1, pts), jnp.float32)], axis=0)
    load = jnp.concatenate([grads, copies(tail, nz)], axis=1)
    load = copies(load, n["y0"]).reshape(n["y0"] * nz, 3 * rows + TAIL, pts)
    own = lax.all_to_all(load, ("y0", "h", "l"), 0, 0, tiled=True)
    values, own = lax.optimization_barrier((values, own))
    other = lax.ppermute(own, "c", SWAP)

    near = own[:, 3 * rows + 3 : 3 * rows + 3 + 3 * n["yh"], :].reshape(n["y0"], nz, n["yh"], 3, pts)
    near = lax.dynamic_index_in_dim(near, lax.axis_index("y0"), 0, False)
    src = near.transpose(1, 2, 0, 3).reshape(n["yh"], 3, nz * pts)
    src = jnp.pad(src, ((0, 0), (0, 5), (0, 0)))
    origin = jnp.broadcast_to(jnp.mean(src, axis=(0, 2))[:, None], (8, pts))

    values = with_layout_constraint(lax.all_to_all(values, ("h", "l"), 0, 0, tiled=True), rowmajor)

    partial_z = pair_matmul(origin, own, other, src)
    spts = partial_z.shape[2]
    values = values.transpose(1, 0, 2).reshape(slab, spts)
    partial_z, values, south = lax.optimization_barrier((partial_z, values, c == 0))

    arrived = lax.all_to_all(partial_z, "yh", 0, 0, tiled=True)
    z = arrived.sum(axis=0).reshape(n["c"], piece, spts)
    z = jnp.where(south, z, z[::-1]).reshape(rows, spts)
    z_all = lax.all_to_all(copies(z, nv), VEC, 0, 0, tiled=True).reshape(nv, n["c"], piece, spts)

    def product(k):
        zc = z_all[:, k].reshape(nv * piece, spts)
        return lax.dot_general(zc, values, (((1,), (1,)), ((), ())), precision=lax.Precision.HIGH)

    part = lax.ppermute(product(1), "c", SWAP) + product(0)
    back = lax.all_to_all(part.reshape(nv, piece, slab), ("yh", "y0"), 0, 0, tiled=True)
    return back.sum(axis=0)


def solution(mesh):
    fine = Mesh(mesh.devices.reshape(4, 2, 2, 2, 2, 4, 2), GRID + VEC)

    return jax.shard_map(
        body,
        mesh=fine,
        in_specs=(P(None, GRID), P(None, GRID), P(VEC, GRID), P(None, VEC, GRID)),
        out_specs=P(GRID, VEC),
        check_vma=False,
    )
```

```python
import jax
import jax.numpy as jnp
from jax import lax
from jax.experimental.layout import Layout, with_layout_constraint
from jax.experimental import pallas as pl
from jax.experimental.pallas import tpu as pltpu
from jax.sharding import Mesh, PartitionSpec as P


SOFT2 = 0.05 * 0.05
TINY = 1e-30
GRID = ("yh", "y0", "h", "l", "c")
VEC = ("x", "zl")
SWAP = [(0, 1), (1, 0)]
BF16 = jnp.bfloat16
TAIL = 8


def copies(block, peers):
    return jnp.broadcast_to(block[None], (peers,) + block.shape)


def split(a):
    hi = a.astype(BF16)
    return hi, (a - hi.astype(jnp.float32)).astype(BF16)


def times_transposed(a, b):
    return lax.dot_general(a, b, (((1,), (1,)), ((), ())), preferred_element_type=jnp.float32)


def pair_matmul_kernel(first_ref, origin_ref, own_ref, other_ref, src_ref, *rest):
    out_ref, hi_ref, lo_ref = rest[-3:]
    blocks, _, half = own_ref.shape
    rows = out_ref.shape[1]
    origin = [origin_ref[comp : comp + 1, 0:1] for comp in range(3)]

    @pl.when(pl.program_id(0) == 0)
    def _():
        for j in range(blocks):
            for side, ref in enumerate((own_ref, other_ref)):
                cols = slice(side * half, (side + 1) * half)
                moment = None
                for comp in range(3):
                    g = ref[j, comp * rows : (comp + 1) * rows, :]
                    hi, lo = split(g)
                    hi_ref[j, (comp + 1) * rows : (comp + 2) * rows, cols] = hi
                    lo_ref[j, (comp + 1) * rows : (comp + 2) * rows, cols] = lo
                    tgt = ref[j, 3 * rows + comp : 3 * rows + comp + 1, :] - origin[comp]
                    moment = g * tgt if moment is None else moment + g * tgt
                hi, lo = split(moment)
                hi_ref[j, :rows, cols] = hi
                lo_ref[j, :rows, cols] = lo

    src_cols = src_ref[0].T
    src = [src_cols[:, comp : comp + 1] for comp in range(3)]
    total = None
    for j in range(blocks):
        dist2 = None
        for comp in range(3):
            row = slice(3 * rows + comp, 3 * rows + comp + 1)
            tgt = jnp.concatenate([own_ref[j, row, :], other_ref[j, row, :]], axis=1)
            diff = tgt - src[comp]
            dist2 = diff * diff if dist2 is None else dist2 + diff * diff
        grow = 1.0 + dist2 * lax.rsqrt(jnp.maximum(dist2, TINY))
        grow2 = grow * grow
        hi, lo = split(lax.rsqrt((dist2 + SOFT2) * (grow2 * grow2)))
        part = times_transposed(hi, hi_ref[j]) + times_transposed(lo, hi_ref[j]) + times_transposed(hi, lo_ref[j])
        total = part if total is None else total + part
    z = total[:, :rows]
    for comp in range(3):
        z = z - (src[comp] - origin[comp]) * total[:, (comp + 1) * rows : (comp + 2) * rows]
    out_ref[0] = (0.5 * z).T


def pair_matmul(first, origin, own, other, src, peers, *earlier):
    blocks, height, half = own.shape
    rows = (height - TAIL) // 3
    given, _, per = src.shape
    lead = len(earlier)
    steps = peers - 1 if lead else 1
    pairs = steps * per * 2 * half * blocks

    def where(i, f):
        return ((i + lead + f[0]) % peers, 0, 0)

    vmem = pl.BlockSpec(memory_space=pltpu.VMEM)
    return pl.pallas_call(
        pair_matmul_kernel,
        out_shape=jax.ShapeDtypeStruct((peers, rows, per), jnp.float32),
        grid_spec=pltpu.PrefetchScalarGridSpec(
            num_scalar_prefetch=1,
            grid=(steps,),
            in_specs=[vmem] * 3
            + [pl.BlockSpec((1, 8, per), where if given > 1 else lambda i, f: (0, 0, 0))]
            + [pl.BlockSpec(memory_space=pl.ANY)] * lead,
            out_specs=pl.BlockSpec((1, rows, per), where),
            scratch_shapes=[pltpu.VMEM((blocks, 4 * rows, 2 * half), BF16)] * 2,
        ),
        input_output_aliases={5: 0} if lead else {},
        compiler_params=pltpu.CompilerParams(
            dimension_semantics=("arbitrary",), vmem_limit_bytes=32 * 1024 * 1024
        ),
        cost_estimate=pl.CostEstimate(
            flops=pairs * 4 * rows * 2 * 3,
            bytes_accessed=2 * blocks * height * half * 4 + steps * rows * per * 4,
            transcendentals=2 * pairs,
        ),
    )(first, origin, own, other, src, *earlier)


def origin_of(src):
    return jnp.broadcast_to(jnp.mean(src, axis=(0, 2))[:, None], (8, 128))


def body(tgt_coords, src_coords, src_values, grad_vectors):
    n = {a: lax.axis_size(a) for a in GRID + VEC}
    nz = n["h"] * n["l"]
    nv = n["x"] * n["zl"]
    slab, pts = src_values.shape
    rows = slab // nz
    piece = rows // n["c"]
    c = lax.axis_index("c")

    rowmajor = Layout(major_to_minor=(0, 1, 2))
    values = with_layout_constraint(copies(src_values, nz), rowmajor)

    grads = grad_vectors.reshape(3, nz, rows, pts).transpose(1, 0, 2, 3).reshape(nz, 3 * rows, pts)
    tail = jnp.concatenate([tgt_coords, src_coords, jnp.zeros((TAIL - 6, pts), jnp.float32)], axis=0)
    load = jnp.concatenate([grads, copies(tail, nz)], axis=1)
    load = copies(load, n["y0"]).reshape(n["y0"] * nz, 3 * rows + TAIL, pts)
    own = lax.all_to_all(load, ("y0", "h", "l"), 0, 0, tiled=True)
    other = lax.ppermute(own, "c", SWAP)

    near = own[:, 3 * rows + 3 : 3 * rows + 6, :].reshape(n["y0"], nz, 3, pts)
    near = lax.dynamic_index_in_dim(near, lax.axis_index("y0"), 0, False)
    near = jnp.pad(near.transpose(1, 0, 2).reshape(3, nz * pts), ((0, 5), (0, 0)))
    first = lax.axis_index("yh").astype(jnp.int32).reshape(1)
    src = lax.all_to_all(copies(near, n["yh"]), "yh", 0, 0, tiled=True)
    partial_z = pair_matmul(first, origin_of(near[None]), own, other, near[None], n["yh"])
    src, values, partial_z = lax.optimization_barrier((src, values, partial_z))

    values = with_layout_constraint(lax.all_to_all(values, ("h", "l"), 0, 0, tiled=True), rowmajor)

    partial_z = pair_matmul(first, origin_of(src), own, other, src, n["yh"], partial_z)
    spts = partial_z.shape[2]
    values = values.transpose(1, 0, 2).reshape(slab, spts)
    partial_z, values, south = lax.optimization_barrier((partial_z, values, c == 0))

    arrived = lax.all_to_all(partial_z, "yh", 0, 0, tiled=True)
    z = arrived.sum(axis=0).reshape(n["c"], piece, spts)
    z = jnp.where(south, z, z[::-1]).reshape(rows, spts)
    z_all = lax.all_to_all(copies(z, nv), VEC, 0, 0, tiled=True).reshape(nv, n["c"], piece, spts)

    def product(k):
        zc = z_all[:, k].reshape(nv * piece, spts)
        return lax.dot_general(zc, values, (((1,), (1,)), ((), ())), precision=lax.Precision.HIGH)

    part = lax.ppermute(product(1), "c", SWAP) + product(0)
    back = lax.all_to_all(part.reshape(nv, piece, slab), ("yh", "y0"), 0, 0, tiled=True)
    return back.sum(axis=0)


def solution(mesh):
    fine = Mesh(mesh.devices.reshape(4, 2, 2, 2, 2, 4, 2), GRID + VEC)

    return jax.shard_map(
        body,
        mesh=fine,
        in_specs=(P(None, GRID), P(None, GRID), P(VEC, GRID), P(None, VEC, GRID)),
        out_specs=P(GRID, VEC),
        check_vma=False,
    )
```

```python
import jax
import jax.numpy as jnp
from jax import lax
from jax.experimental.layout import Layout, with_layout_constraint
from jax.experimental import pallas as pl
from jax.experimental.pallas import tpu as pltpu
from jax.sharding import Mesh, PartitionSpec as P


SOFT2 = 0.05 * 0.05
TINY = 1e-30
GRID = ("yh", "y0", "h", "l", "c")
VEC = ("x", "zl")
SWAP = [(0, 1), (1, 0)]
BF16 = jnp.bfloat16
TAIL = 16


def copies(block, peers):
    return jnp.broadcast_to(block[None], (peers,) + block.shape)


def split(a):
    hi = a.astype(BF16)
    return hi, (a - hi.astype(jnp.float32)).astype(BF16)


def times_transposed(a, b):
    return lax.dot_general(a, b, (((1,), (1,)), ((), ())), preferred_element_type=jnp.float32)


def pair_matmul_kernel(origin_ref, own_ref, other_ref, src_ref, out_ref, hi_ref, lo_ref):
    blocks, _, half = own_ref.shape
    rows = out_ref.shape[1]
    origin = [origin_ref[comp : comp + 1, 0:1] for comp in range(3)]

    @pl.when(pl.program_id(0) == 0)
    def _():
        for j in range(blocks):
            for side, ref in enumerate((own_ref, other_ref)):
                cols = slice(side * half, (side + 1) * half)
                moment = None
                for comp in range(3):
                    g = ref[j, comp * rows : (comp + 1) * rows, :]
                    hi, lo = split(g)
                    hi_ref[j, (comp + 1) * rows : (comp + 2) * rows, cols] = hi
                    lo_ref[j, (comp + 1) * rows : (comp + 2) * rows, cols] = lo
                    tgt = ref[j, 3 * rows + comp : 3 * rows + comp + 1, :] - origin[comp]
                    moment = g * tgt if moment is None else moment + g * tgt
                hi, lo = split(moment)
                hi_ref[j, :rows, cols] = hi
                lo_ref[j, :rows, cols] = lo

    src_cols = src_ref[0].T
    src = [src_cols[:, comp : comp + 1] for comp in range(3)]
    total = None
    for j in range(blocks):
        dist2 = None
        for comp in range(3):
            row = slice(3 * rows + comp, 3 * rows + comp + 1)
            tgt = jnp.concatenate([own_ref[j, row, :], other_ref[j, row, :]], axis=1)
            diff = tgt - src[comp]
            dist2 = diff * diff if dist2 is None else dist2 + diff * diff
        grow = 1.0 + dist2 * lax.rsqrt(jnp.maximum(dist2, TINY))
        grow2 = grow * grow
        hi, lo = split(lax.rsqrt((dist2 + SOFT2) * (grow2 * grow2)))
        part = times_transposed(hi, hi_ref[j]) + times_transposed(lo, hi_ref[j]) + times_transposed(hi, lo_ref[j])
        total = part if total is None else total + part
    z = total[:, :rows]
    for comp in range(3):
        z = z - (src[comp] - origin[comp]) * total[:, (comp + 1) * rows : (comp + 2) * rows]
    out_ref[0] = (0.5 * z).T


def pair_matmul(origin, own, other, src):
    blocks, height, half = own.shape
    rows = (height - TAIL) // 3
    peers, _, per = src.shape
    pairs = peers * per * 2 * half * blocks
    return pl.pallas_call(
        pair_matmul_kernel,
        out_shape=jax.ShapeDtypeStruct((peers, rows, per), jnp.float32),
        grid=(peers,),
        in_specs=[pl.BlockSpec(memory_space=pltpu.VMEM)] * 3 + [pl.BlockSpec((1, 8, per), lambda i: (i, 0, 0))],
        out_specs=pl.BlockSpec((1, rows, per), lambda i: (i, 0, 0)),
        scratch_shapes=[pltpu.VMEM((blocks, 4 * rows, 2 * half), BF16)] * 2,
        compiler_params=pltpu.CompilerParams(
            dimension_semantics=("arbitrary",), vmem_limit_bytes=32 * 1024 * 1024
        ),
        cost_estimate=pl.CostEstimate(
            flops=pairs * 4 * rows * 2 * 3,
            bytes_accessed=2 * blocks * height * half * 4 + peers * rows * per * 4,
            transcendentals=2 * pairs,
        ),
    )(origin, own, other, src)


def body(tgt_coords, src_coords, src_values, grad_vectors):
    n = {a: lax.axis_size(a) for a in GRID + VEC}
    nz = n["h"] * n["l"]
    nv = n["x"] * n["zl"]
    slab, pts = src_values.shape
    rows = slab // nz
    piece = rows // n["c"]
    c = lax.axis_index("c")

    src_y = lax.all_to_all(copies(src_coords, n["yh"]), "yh", 0, 0, tiled=True)
    src_y = src_y.reshape(3 * n["yh"], pts)
    rowmajor = Layout(major_to_minor=(0, 1, 2))
    values = with_layout_constraint(copies(src_values, nz), rowmajor)

    grads = grad_vectors.reshape(3, nz, rows, pts).transpose(1, 0, 2, 3).reshape(nz, 3 * rows, pts)
    tail = jnp.concatenate([tgt_coords, src_y, jnp.zeros((1, pts), jnp.float32)], axis=0)
    load = jnp.concatenate([grads, copies(tail, nz)], axis=1)
    own = lax.all_to_all(load, ("h", "l"), 0, 0, tiled=True)
    far = lax.ppermute(own, "y0", SWAP)
    near = own[:, 3 * rows + 3 : 3 * rows + 3 + 3 * n["yh"], :].reshape(nz, n["yh"], 3, pts)
    values, near = lax.optimization_barrier((values, near))
    own = jnp.concatenate([own, far], axis=0)
    other = lax.ppermute(own, "c", SWAP)
    src = near.transpose(1, 2, 0, 3).reshape(n["yh"], 3, nz * pts)
    src = jnp.pad(src, ((0, 0), (0, 5), (0, 0)))
    origin = jnp.broadcast_to(jnp.mean(src, axis=(0, 2))[:, None], (8, pts))

    values = with_layout_constraint(lax.all_to_all(values, ("h", "l"), 0, 0, tiled=True), rowmajor)

    partial_z = pair_matmul(origin, own, other, src)
    spts = partial_z.shape[2]
    values = values.transpose(1, 0, 2).reshape(slab, spts)
    partial_z, values, south = lax.optimization_barrier((partial_z, values, c == 0))

    arrived = lax.all_to_all(partial_z, "yh", 0, 0, tiled=True)
    z = arrived.sum(axis=0).reshape(n["c"], piece, spts)
    z = jnp.where(south, z, z[::-1]).reshape(rows, spts)
    z_all = lax.all_to_all(copies(z, nv), VEC, 0, 0, tiled=True).reshape(nv, n["c"], piece, spts)

    def product(k):
        zc = z_all[:, k].reshape(nv * piece, spts)
        return lax.dot_general(zc, values, (((1,), (1,)), ((), ())), precision=lax.Precision.HIGH)

    part = lax.ppermute(product(1), "c", SWAP) + product(0)
    back = lax.all_to_all(part.reshape(nv, piece, slab), ("yh", "y0"), 0, 0, tiled=True)
    return back.sum(axis=0)


def solution(mesh):
    fine = Mesh(mesh.devices.reshape(4, 2, 2, 2, 2, 4, 2), GRID + VEC)

    return jax.shard_map(
        body,
        mesh=fine,
        in_specs=(P(None, GRID), P(None, GRID), P(VEC, GRID), P(None, VEC, GRID)),
        out_specs=P(GRID, VEC),
        check_vma=False,
    )
```
